32 devices in a mesh: groups: 2 (over y), seq: 4 (over z), fsdp: 2 (over x), sub: 2 (over core).
Axes of the slice: x: 2, y: 2, z: 4, core: 2. Of those that a mesh axis runs over, the one named last changes fastest.
Arguments:
- tokens: bfloat16 [2048, 8192], P(('groups', 'seq')), parts along dimension 0, may hold values from -400 to 400
- norm_gain: float32 [8192], replicated, may hold values from 0.1 to 1.9
- w_query: bfloat16 [8, 16, 8192], P(('seq', 'sub'), 'fsdp'), may hold values from -0.0625 to 0.0625
- w_key: bfloat16 [8, 16, 8192], P(('seq', 'sub'), 'fsdp'), may hold values from -0.0625 to 0.0625
- w_value: bfloat16 [8, 128, 8192], P(('seq', 'sub'), 'fsdp'), may hold values from -5 to 5
- head_gain: float32 [128], replicated, may hold values from 0.1 to 1.9
- w_out: bfloat16 [8, 128, 8192], P('seq', None, ('fsdp', 'sub')), may hold values from -0.1875 to 0.1875
Outputs:
- mixed: bfloat16 [2048, 8192], P(('groups', 'seq'), ('fsdp', 'sub')), parts along dimension 0
The draws below stay inside these ranges and needn't reach their ends.
There are 2 independent parts, one for each index of `groups`. The reference program is written for one: setup_inputs(seed, part) draws one part's arguments, and reference() takes and returns one part's arrays. A program takes and returns all parts, laid end to end along the dimension named above; an argument that names none is the same for every part. Nothing has to cross between parts.
All inputs are finite; a program needn't handle non-finite values.
Results may differ from the reference program's by a relative error of at most 0.0084.
Values may be sent and summed in bfloat16 or wider, within the bound.
A program may use at most 64 MiB of HBM per device.

```python
import math
import jax
import jax.numpy as jnp
import numpy as np
from jax import lax

D = 8192
HEAD_DIM = 128
FEAT = 16
BLOCK = 512
HEADS = 8
L = 1024


def draw_tokens(key, part):
    subkeys = jax.random.split(jax.random.fold_in(key, 101), 3)
    row_scale = jnp.exp(jax.random.uniform(subkeys[0], (L, 1), jnp.float32, 0.0, math.log(10.0)))
    col_scale = jnp.exp(jax.random.uniform(subkeys[1], (1, D), jnp.float32, 0.0, math.log(10.0)))
    entries = jnp.clip(jax.random.normal(subkeys[2], (L, D), jnp.float32), -4.0, 4.0)
    return (entries * row_scale * col_scale).astype(jnp.bfloat16)


def draw_w_value(key, part):
    subkeys = jax.random.split(jax.random.fold_in(key, 202), 2)
    upward = jnp.arange(HEAD_DIM, dtype=jnp.float32)[None, :, None] / (HEAD_DIM - 1.0)
    jitter = jax.random.uniform(subkeys[0], (HEADS, HEAD_DIM, 1), jnp.float32, 0.0, 1.0)
    exponent = 0.5 * upward + 0.5 * jitter
    entries = jnp.clip(jax.random.normal(subkeys[1], (HEADS, HEAD_DIM, D), jnp.float32), -4.0, 4.0)
    factor = jnp.power(10.0, exponent) / math.sqrt(D)
    return (entries * factor).astype(jnp.bfloat16)


def levels(key, extent, cuts, low, top_value):
    gain, own = 1.0, jax.random.fold_in(key, 6)
    for position, parts in cuts:
        draws = jnp.exp(jax.random.uniform(jax.random.fold_in(own, position), (parts,), jnp.float32, low / len(cuts), top_value / len(cuts)))
        gain = gain * jnp.repeat(draws, extent[position] // parts).reshape([-1 if axis == position else 1 for axis in range(len(extent))])
    return gain


def centred(own_key, dims, width, limit, cuts=(), kind=jnp.bfloat16):
    drawn = jax.random.normal(own_key, dims, jnp.float32) * width
    if len(cuts) > 0:
        drawn = levels(own_key, dims, cuts, -0.22, 0.18) * drawn
    return jnp.clip(drawn, min=-limit, max=limit).astype(kind)


def setup_inputs(seed: int = 0, part: int = 0) -> dict:
    key_list = jax.random.split(jax.random.key(seed), 8)
    own_keys = jax.random.split(jax.random.fold_in(key_list[7], part), 8)
    tokens = draw_tokens(jax.random.fold_in(jax.random.fold_in(key_list[7], part), 71), part)
    norm_gain = jnp.clip(1.0 + 0.18 * jax.random.normal(key_list[1], (D,), jnp.float32), 0.1, 1.9)
    w_query = centred(key_list[2], (HEADS, FEAT, D), D ** -0.5, 0.0625, ((0, 8), (1, 2)))
    w_key = centred(key_list[3], (HEADS, FEAT, D), D ** -0.5, 0.0625, ((0, 8), (1, 2)))
    w_value = draw_w_value(jax.random.fold_in(key_list[7], 71), part)
    head_gain = jnp.clip(1.0 + 0.18 * jax.random.normal(key_list[5], (HEAD_DIM,), jnp.float32), 0.1, 1.9)
    w_out = centred(key_list[6], (HEADS, HEAD_DIM, D), (HEADS * HEAD_DIM) ** -0.5, 0.1875, ((0, 4), (2, 4)))
    return dict(tokens=tokens, norm_gain=norm_gain, w_query=w_query, w_key=w_key, w_value=w_value, head_gain=head_gain, w_out=w_out)


def taylor_last(vectors):
    feature_count = vectors.shape[-1]
    first_row, second_row = np.triu_indices(feature_count, 1)
    cross_terms = vectors[..., first_row] * vectors[..., second_row] / 4.0
    squares = vectors * vectors / (4.0 * math.sqrt(2.0))
    leading = jnp.ones(vectors.shape[:-1] + (1,), jnp.float32)
    return jnp.concatenate([leading, vectors / 2.0, cross_terms, squares], -1)

def reference(tokens, norm_gain, w_query, w_key, w_value, head_gain, w_out):
    inputs = tokens.astype(jnp.float32)
    meansq = lax.optimization_barrier(jnp.mean(inputs * inputs, axis=-1, keepdims=True))
    normed = (inputs * lax.rsqrt(meansq + 1e-05) * norm_gain).astype(jnp.bfloat16)
    length = tokens.shape[0]

    def project(weight):
        flattened = weight.reshape(-1, weight.shape[-1])
        result = jnp.dot(normed, flattened.T, preferred_element_type=jnp.float32)
        result = result.astype(jnp.bfloat16).reshape(length, weight.shape[0], weight.shape[1])
        return jnp.transpose(result, (1, 0, 2))
    queries = project(w_query)
    key_vectors = project(w_key)
    values_all = project(w_value)
    nblocks = length // BLOCK
    position_t = jnp.arange(BLOCK, dtype=jnp.int32)[:, None]
    position_j = jnp.arange(BLOCK, dtype=jnp.int32)[None, :]
    causal = position_j <= position_t

    def one_head(operands):
        head_query, head_key, head_value = operands
        query_feats = taylor_last(head_query.astype(jnp.float32)).astype(jnp.bfloat16)
        key_feats = taylor_last(head_key.astype(jnp.float32)).astype(jnp.bfloat16)
        key_blocks = key_feats.astype(jnp.float32).reshape(nblocks, BLOCK, -1)
        value_blocks = head_value.astype(jnp.float32).reshape(nblocks, BLOCK, -1)
        contrib = jnp.einsum('bjf,bje->bfe', key_blocks, value_blocks)
        prefix = jnp.concatenate([jnp.zeros_like(contrib[:1]), jnp.cumsum(contrib[:-1], axis=0)], 0)
        prior_state = prefix.astype(jnp.bfloat16)
        query_blocks = head_query.astype(jnp.float32).reshape(nblocks, BLOCK, -1)
        raw_keys = head_key.astype(jnp.float32).reshape(nblocks, BLOCK, -1)
        scores = jnp.einsum('btf,bjf->btj', query_blocks, raw_keys)
        kernel = 1.0 + scores / 4.0 + scores * scores / 32.0
        weight = jnp.where(causal[None], kernel, 0.0).astype(jnp.bfloat16)
        local_part = jnp.einsum('btj,bje->bte', weight.astype(jnp.float32), value_blocks)
        feat_blocks = query_feats.astype(jnp.float32).reshape(nblocks, BLOCK, -1)
        carried = jnp.einsum('btf,bfe->bte', feat_blocks, prior_state.astype(jnp.float32))
        return (local_part + carried).reshape(length, -1).astype(jnp.bfloat16)
    numerator = lax.map(one_head, (queries, key_vectors, values_all))
    widened = numerator.astype(jnp.float32)
    meansq_out = lax.optimization_barrier(jnp.mean(widened * widened, axis=-1, keepdims=True))
    attended = (widened * lax.rsqrt(meansq_out + 1e-06) * head_gain).astype(jnp.bfloat16)
    flat_att = jnp.transpose(attended, (1, 0, 2)).reshape(length, -1)
    out_rows = w_out.reshape(-1, w_out.shape[-1])
    return jnp.dot(flat_att, out_rows, preferred_element_type=jnp.float32).astype(jnp.bfloat16)
```

```python
import functools

import jax
import jax.numpy as jnp
from jax import lax
from jax.experimental import pallas as pl
from jax.experimental.pallas import tpu as pltpu
from jax.sharding import PartitionSpec as P

MESH = pl.DeviceIdType.MESH
F32 = jnp.float32
BF16 = jnp.bfloat16


def kernel(
    n,
    nf,
    ns,
    pieces,
    out_pieces,
    tok_ref,
    gain_ref,
    w_ref,
    head_gain_ref,
    wo_ref,
    out_ref,
    normed,
    wbuf,
    wobuf,
    qk_send,
    v_send,
    qk_all,
    v_all,
    q_full,
    k_full,
    num_send,
    num_all,
    attended,
    total,
    w_zrecv,
    w_yrecv,
    w_right,
    w_left,
    w_across,
    o_zrecv,
    o_yrecv,
    o_right,
    o_left,
    o_across,
    qk_ssem,
    qk_rsem,
    v_ssem,
    v_rsem,
    num_ssem,
    num_rsem,
    sib_ssem,
    sib_rsem,
):
    group = lax.axis_index("groups")
    me = lax.axis_index("seq")
    my_f = lax.axis_index("fsdp")
    my_s = lax.axis_index("sub")
    tokens, width = tok_ref.shape
    span = width // (2 * pieces)
    qk_rows = qk_all.shape[2]
    half_rows = qk_rows // 2

    def own_w(c):
        start = pl.multiple_of((group * pieces + c) * span, span)
        return w_ref.at[:, pl.ds(start, span)]

    def own_o(c):
        return wo_ref.at[group, c]

    class Stream:
        def __init__(self, own, buf, count, zrecv, yrecv, right, left, across):
            self.own, self.buf, self.count = own, buf, count
            self.zrecv, self.yrecv = zrecv, yrecv
            self.right_sem, self.left_sem, self.across_sem = right, left, across

        def along(self, o, c, sems, target, own):
            slot = self.buf.at[o, group, c]
            return pltpu.make_async_remote_copy(
                src_ref=self.own(c) if own else slot,
                dst_ref=slot,
                send_sem=sems.at[o, c],
                recv_sem=self.zrecv.at[o, c],
                device_id={"seq": target},
                device_id_type=MESH,
            )

        def right(self, o, c, own=False):
            return self.along(o, c, self.right_sem, me + 1, own)

        def left(self, o, c, own=False):
            return self.along(o, c, self.left_sem, me - 1, own)

        def across(self, o, c, half):
            slot = self.buf.at[o, half, c]
            return pltpu.make_async_remote_copy(
                src_ref=slot,
                dst_ref=slot,
                send_sem=self.across_sem.at[o, c],
                recv_sem=self.yrecv.at[o, c],
                device_id={"groups": 1 - group},
                device_id_type=MESH,
            )

        def begin(self):
            for c in range(self.count):

                @pl.when(me + 1 < n)
                def _():
                    self.right(me, c, True).start()

                @pl.when(me >= 1)
                def _():
                    self.left(me, c, True).start()

        def relay(self, r):
            for c in range(self.count):

                @pl.when(me >= r)
                def _():
                    o = me - r
                    self.right(o, c).wait_recv()

                    @pl.when(me + 1 < n)
                    def _():
                        self.right(o, c).start()

                    self.across(o, c, group).start()

                @pl.when(me + r < n)
                def _():
                    o = me + r
                    self.left(o, c).wait_recv()

                    @pl.when(me >= 1)
                    def _():
                        self.left(o, c).start()

                    self.across(o, c, group).start()

        def arrive(self, o):
            for c in range(self.count):
                self.across(o, c, 1 - group).wait_recv()

        def finish(self):
            for r in range(n):
                for c in range(self.count):

                    @pl.when((me >= r) & (me + 1 < n))
                    def _():
                        self.right(me - r, c, r == 0).wait_send()

                    @pl.when((me + r < n) & (me >= 1))
                    def _():
                        self.left(me + r, c, r == 0).wait_send()

                    if r > 0:

                        @pl.when(me >= r)
                        def _():
                            self.across(me - r, c, group).wait_send()

                        @pl.when(me + r < n)
                        def _():
                            self.across(me + r, c, group).wait_send()

    w_stream = Stream(own_w, wbuf, pieces, w_zrecv, w_yrecv, w_right, w_left, w_across)
    o_stream = Stream(own_o, wobuf, out_pieces, o_zrecv, o_yrecv, o_right, o_left, o_across)

    w_stream.begin()

    row_step = 16

    def norm_rows(i, carry):
        rows = pl.ds(pl.multiple_of(i * row_step, row_step), row_step)
        sumsq = jnp.zeros((row_step, 1), F32)
        for c in range(2 * pieces):
            part = tok_ref[rows, c * span : (c + 1) * span].astype(F32)
            sumsq = sumsq + jnp.sum(part * part, axis=1, keepdims=True)
        scale = lax.rsqrt(sumsq / width + 1e-05)
        for c in range(2 * pieces):
            cols = slice(c * span, (c + 1) * span)
            part = tok_ref[rows, cols].astype(F32)
            normed[c, rows, :] = (part * scale * gain_ref[:, cols]).astype(BF16)
        return carry

    lax.fori_loop(0, tokens // row_step, norm_rows, 0)

    def contract(weights, acts):
        return lax.dot_general(weights, acts, (((1,), (1,)), ((), ())), preferred_element_type=F32)

    def qk_copy(o, source, other_f, token_block, f_from):
        return pltpu.make_async_remote_copy(
            src_ref=source,
            dst_ref=qk_all.at[token_block, f_from],
            send_sem=qk_ssem.at[o, other_f],
            recv_sem=qk_rsem.at[token_block, f_from],
            device_id={"seq": o, "fsdp": other_f},
            device_id_type=MESH,
        )

    def v_copy(o, token_block):
        return pltpu.make_async_remote_copy(
            src_ref=v_send.at[o],
            dst_ref=v_all.at[token_block],
            send_sem=v_ssem.at[o],
            recv_sem=v_rsem.at[token_block],
            device_id={"seq": o},
            device_id_type=MESH,
        )

    def project_own():
        acc = jnp.zeros((w_ref.shape[0], tokens), F32)
        for c in range(2 * pieces):
            acc = acc + contract(w_ref[:, c * span : (c + 1) * span], normed[c])
        qk_all[me, my_f] = acc[:qk_rows].astype(BF16)
        v_all[me] = acc[qk_rows:].astype(BF16)
        for df in range(1, nf):
            other = lax.rem(my_f + df, nf)
            qk_copy(me, qk_all.at[me, my_f], other, me, my_f).start()

    def project(o):
        def body(c, acc):
            return acc + contract(wbuf[o, c // pieces, c % pieces], normed[c])

        acc = lax.fori_loop(0, 2 * pieces, body, jnp.zeros((w_ref.shape[0], tokens), F32))
        qk_send[o] = acc[:qk_rows].astype(BF16)
        v_send[o] = acc[qk_rows:].astype(BF16)
        for df in range(nf):
            qk_copy(o, qk_send.at[o], lax.rem(my_f + df, nf), me, my_f).start()
        v_copy(o, me).start()

    def both(r, action):
        @pl.when(me >= r)
        def _():
            action(me - r)

        @pl.when(me + r < n)
        def _():
            action(me + r)

    def take(o):
        w_stream.arrive(o)
        project(o)

    project_own()
    for r in range(1, n):
        w_stream.relay(r)
        if r > 1:
            both(r - 1, take)
    o_stream.begin()
    both(n - 1, take)

    o_stream.relay(1)

    for d in range(1, n):
        t = lax.rem(me + d, n)
        v_copy(me, t).wait_recv()
        for df in range(nf):
            qk_copy(me, qk_all.at[t, df], 0, t, df).wait_recv()
    for df in range(1, nf):
        other = lax.rem(my_f + df, nf)
        qk_copy(me, qk_all.at[me, other], other, me, other).wait_recv()

    for t in range(n):
        parts = [qk_all[t, f].astype(F32) for f in range(nf)]
        q_full[t] = jnp.concatenate([p[:half_rows] for p in parts], 0).astype(BF16)
        k_full[t] = jnp.concatenate([p[half_rows:] for p in parts], 0).astype(BF16)

    channels = v_all.shape[1]
    key_pos = lax.broadcasted_iota(jnp.int32, (tokens, tokens), 0)
    query_pos = lax.broadcasted_iota(jnp.int32, (tokens, tokens), 1)

    def numerator(t):
        queries = q_full[t]

        def body(j, acc):
            scores = lax.dot_general(
                k_full[j], queries, (((0,), (0,)), ((), ())), preferred_element_type=F32
            )
            value = 1.0 + scores * 0.25 + scores * scores * 0.03125
            weight = jnp.where(key_pos + (j - t) * tokens <= query_pos, value, 0.0).astype(BF16)
            return acc + jnp.dot(v_all[j], weight, preferred_element_type=F32)

        acc = lax.fori_loop(0, t + 1, body, jnp.zeros((channels, tokens), F32))
        return acc.astype(BF16)

    def num_copy(t, head_block):
        return pltpu.make_async_remote_copy(
            src_ref=num_send.at[t],
            dst_ref=num_all.at[head_block, my_f, my_s],
            send_sem=num_ssem.at[t],
            recv_sem=num_rsem.at[head_block],
            device_id={"seq": t},
            device_id_type=MESH,
        )

    def sib_copy(o, to_f, to_s, from_f, from_s):
        slot = num_all.at[o, from_f, from_s]
        return pltpu.make_async_remote_copy(
            src_ref=slot,
            dst_ref=slot,
            send_sem=sib_ssem.at[o, to_f, to_s],
            recv_sem=sib_rsem.at[o, from_f, from_s],
            device_id={"fsdp": to_f, "sub": to_s},
            device_id_type=MESH,
        )

    def siblings():
        for df in range(nf):
            for ds in range(ns):
                if df or ds:
                    yield lax.rem(my_f + df, nf), lax.rem(my_s + ds, ns)

    for d in range(1, n):
        t = lax.rem(me + d, n)
        num_send[t] = numerator(t)
        num_copy(t, me).start()
    num_all[me, my_f, my_s] = numerator(me)
    for f, s in siblings():
        sib_copy(me, f, s, my_f, my_s).start()

    for r in range(2, n):
        o_stream.relay(r)
        if r == 2:
            for d in range(1, n):
                o = lax.rem(me + d, n)
                num_copy(o, o).wait_recv()
                for f, s in siblings():
                    sib_copy(o, f, s, my_f, my_s).start()

    for d in range(n):
        o = lax.rem(me + d, n)
        for f, s in siblings():
            sib_copy(o, f, s, f, s).wait_recv()

    head_width = nf * channels

    def attend_block(o, carry):
        for s in range(ns):
            whole = jnp.concatenate([num_all[o, f, s] for f in range(nf)], 0).astype(F32)
            meansq = jnp.sum(whole * whole, axis=0, keepdims=True) / head_width
            scaled = whole * lax.rsqrt(meansq + 1e-06) * head_gain_ref[...]
            attended[o, :, s * head_width : (s + 1) * head_width] = scaled.T.astype(BF16)
        return carry

    lax.fori_loop(0, n, attend_block, 0)

    columns = out_ref.shape[1]
    depth = ns * head_width

    total[...] = jnp.dot(
        attended[me], wo_ref[...].reshape(depth, columns), preferred_element_type=F32
    )

    def multiply(o):
        o_stream.arrive(o)
        total[...] += jnp.dot(
            attended[o], wobuf[o].reshape(depth, columns), preferred_element_type=F32
        )

    for r in range(1, n):
        both(r, multiply)
    out_ref[...] = total[...].astype(BF16)

    w_stream.finish()
    o_stream.finish()
    for d in range(n):
        o = lax.rem(me + d, n)
        for df in range(nf):
            if d or df:
                other = lax.rem(my_f + df, nf)
                source = qk_send.at[o] if d else qk_all.at[me, my_f]
                qk_copy(o, source, other, me, my_f).wait_send()
        if d:
            v_copy(o, me).wait_send()
            num_copy(o, me).wait_send()
        for f, s in siblings():
            sib_copy(o, f, s, my_f, my_s).wait_send()


def per_device(sizes, tokens, norm_gain, w_query, w_key, w_value, head_gain, w_out):
    n, nf, ns = sizes
    stacked = jnp.concatenate([w_query[0], w_key[0], w_value[0]], 0)
    rows, width = stacked.shape
    count = tokens.shape[0]
    qk_rows = w_query.shape[1] + w_key.shape[1]
    channels = w_value.shape[1]
    head_width, columns = w_out.shape[1], w_out.shape[2]
    pieces = max(1, 16 // n)
    out_pieces = max(1, 16 // n)
    wo = w_out.reshape(ns, out_pieces, head_width // out_pieces, columns)
    vmem = pl.BlockSpec(memory_space=pltpu.VMEM)
    dma = pltpu.SemaphoreType.DMA
    return pl.pallas_call(
        functools.partial(kernel, n, nf, ns, pieces, out_pieces),
        out_shape=jax.ShapeDtypeStruct((count, columns), BF16),
        in_specs=[vmem] * 5,
        out_specs=vmem,
        scratch_shapes=[
            pltpu.VMEM((2 * pieces, count, width // (2 * pieces)), BF16),
            pltpu.VMEM((n, 2, pieces, rows, width // (2 * pieces)), BF16),
            pltpu.VMEM((n,) + wo.shape, BF16),
            pltpu.VMEM((n, qk_rows, count), BF16),
            pltpu.VMEM((n, channels, count), BF16),
            pltpu.VMEM((n, nf, qk_rows, count), BF16),
            pltpu.VMEM((n, channels, count), BF16),
            pltpu.VMEM((n, nf * qk_rows // 2, count), BF16),
            pltpu.VMEM((n, nf * qk_rows // 2, count), BF16),
            pltpu.VMEM((n, channels, count), BF16),
            pltpu.VMEM((n, nf, ns, channels, count), BF16),
            pltpu.VMEM((n, count, ns * head_width), BF16),
            pltpu.VMEM((count, columns), F32),
        ]
        + [dma((n, pieces))] * 5
        + [dma((n, out_pieces))] * 5
        + [
            dma((n, nf)),
            dma((n, nf)),
            dma((n,)),
            dma((n,)),
            dma((n,)),
            dma((n,)),
            dma((n, nf, ns)),
            dma((n, nf, ns)),
        ],
        compiler_params=pltpu.CompilerParams(
            has_side_effects=True, vmem_limit_bytes=60 * 1024 * 1024
        ),
    )(tokens, norm_gain.reshape(1, -1), stacked, head_gain.reshape(-1, 1), wo)


def solution(mesh):
    in_specs = (
        P(("groups", "seq"), None),
        P(),
        P(("seq", "sub"), "fsdp", None),
        P(("seq", "sub"), "fsdp", None),
        P(("seq", "sub"), "fsdp", None),
        P(),
        P("seq", None, ("fsdp", "sub")),
    )
    out_specs = P(("groups", "seq"), ("fsdp", "sub"))
    sizes = (mesh.shape["seq"], mesh.shape["fsdp"], mesh.shape["sub"])
    return jax.shard_map(
        functools.partial(per_device, sizes),
        mesh=mesh,
        in_specs=in_specs,
        out_specs=out_specs,
        check_vma=False,
    )
```

```python
import functools

import jax
import jax.numpy as jnp
from jax import lax
from jax.experimental import pallas as pl
from jax.experimental.pallas import tpu as pltpu
from jax.sharding import PartitionSpec as P

MESH = pl.DeviceIdType.MESH
F32 = jnp.float32
BF16 = jnp.bfloat16


def kernel(
    n,
    nf,
    ns,
    pieces,
    out_pieces,
    w_count,
    tok_hbm,
    gain_ref,
    head_gain_ref,
    wo_hbm,
    *rest,
):
    kernel_body(
        n, nf, ns, pieces, out_pieces, tok_hbm, gain_ref, head_gain_ref, wo_hbm,
        rest[:w_count], *rest[w_count:]
    )


def kernel_body(
    n,
    nf,
    ns,
    pieces,
    out_pieces,
    tok_hbm,
    gain_ref,
    head_gain_ref,
    wo_hbm,
    w_hbm,
    out_ref,
    tok_ref,
    w_ref,
    wo_ref,
    load_sem,
    normed,
    wbuf,
    wobuf,
    qk_send,
    v_send,
    qk_all,
    v_all,
    q_full,
    k_full,
    num_send,
    num_all,
    attended,
    total,
    w_zrecv,
    w_yrecv,
    w_right,
    w_left,
    w_across,
    o_zrecv,
    o_yrecv,
    o_right,
    o_left,
    o_across,
    qk_ssem,
    qk_rsem,
    v_ssem,
    v_rsem,
    num_ssem,
    num_rsem,
    sib_ssem,
    sib_rsem,
):
    group = lax.axis_index("groups")
    me = lax.axis_index("seq")
    my_f = lax.axis_index("fsdp")
    my_s = lax.axis_index("sub")
    tokens, width = tok_ref.shape

    loads = []
    row = 0
    for k, source in enumerate(w_hbm):
        size = source.shape[0]
        target = w_ref.at[pl.ds(row, size)] if len(w_hbm) > 1 else w_ref
        loads.append(pltpu.make_async_copy(source, target, load_sem.at[k]))
        row += size
    tok_load = pltpu.make_async_copy(tok_hbm, tok_ref, load_sem.at[len(w_hbm)])
    wo_load = pltpu.make_async_copy(wo_hbm, wo_ref, load_sem.at[len(w_hbm) + 1])
    for load in loads + [tok_load, wo_load]:
        load.start()

    peers = [
        {"seq": lax.rem(me + dz, n), "fsdp": lax.rem(my_f + df, nf)}
        for dz in range(n)
        for df in range(nf)
        if dz or df
    ]
    peers += [
        {"fsdp": lax.rem(my_f + df, nf), "sub": lax.rem(my_s + ds, ns)}
        for df in range(nf)
        for ds in range(1, ns)
    ]
    peers += [{"groups": 1 - group}]
    barrier = pltpu.get_barrier_semaphore()
    for peer in peers:
        pl.semaphore_signal(barrier, inc=1, device_id=peer, device_id_type=MESH)
    pl.semaphore_wait(barrier, len(peers))
    for load in loads:
        load.wait()
    span = width // (2 * pieces)
    qk_rows = qk_all.shape[2]
    half_rows = qk_rows // 2

    def own_w(c):
        start = pl.multiple_of((group * pieces + c) * span, span)
        return w_ref.at[:, pl.ds(start, span)]

    def own_o(c):
        return wo_ref.at[group, c]

    class Stream:
        def __init__(self, own, buf, count, zrecv, yrecv, right, left, across):
            self.own, self.buf, self.count = own, buf, count
            self.zrecv, self.yrecv = zrecv, yrecv
            self.right_sem, self.left_sem, self.across_sem = right, left, across

        def along(self, o, c, sems, target, own):
            slot = self.buf.at[o, group, c]
            return pltpu.make_async_remote_copy(
                src_ref=self.own(c) if own else slot,
                dst_ref=slot,
                send_sem=sems.at[o, c],
                recv_sem=self.zrecv.at[o, c],
                device_id={"seq": target},
                device_id_type=MESH,
            )

        def right(self, o, c, own=False):
            return self.along(o, c, self.right_sem, me + 1, own)

        def left(self, o, c, own=False):
            return self.along(o, c, self.left_sem, me - 1, own)

        def across(self, o, c, half):
            slot = self.buf.at[o, half, c]
            return pltpu.make_async_remote_copy(
                src_ref=slot,
                dst_ref=slot,
                send_sem=self.across_sem.at[o, c],
                recv_sem=self.yrecv.at[o, c],
                device_id={"groups": 1 - group},
                device_id_type=MESH,
            )

        def begin(self):
            for c in range(self.count):

                @pl.when(me + 1 < n)
                def _():
                    self.right(me, c, True).start()

                @pl.when(me >= 1)
                def _():
                    self.left(me, c, True).start()

        def relay(self, r, between=None):
            for c in range(self.count):
                if between is not None and c == self.count // 2:
                    between()

                @pl.when(me >= r)
                def _():
                    o = me - r
                    self.right(o, c).wait_recv()

                    @pl.when(me + 1 < n)
                    def _():
                        self.right(o, c).start()

                    self.across(o, c, group).start()

                @pl.when(me + r < n)
                def _():
                    o = me + r
                    self.left(o, c).wait_recv()

                    @pl.when(me >= 1)
                    def _():
                        self.left(o, c).start()

                    self.across(o, c, group).start()

        def arrive(self, o):
            for c in range(self.count):
                self.across(o, c, 1 - group).wait_recv()

        def finish(self):
            for r in range(n):
                for c in range(self.count):

                    @pl.when((me >= r) & (me + 1 < n))
                    def _():
                        self.right(me - r, c, r == 0).wait_send()

                    @pl.when((me + r < n) & (me >= 1))
                    def _():
                        self.left(me + r, c, r == 0).wait_send()

                    if r > 0:

                        @pl.when(me >= r)
                        def _():
                            self.across(me - r, c, group).wait_send()

                        @pl.when(me + r < n)
                        def _():
                            self.across(me + r, c, group).wait_send()

    w_stream = Stream(own_w, wbuf, pieces, w_zrecv, w_yrecv, w_right, w_left, w_across)
    o_stream = Stream(own_o, wobuf, out_pieces, o_zrecv, o_yrecv, o_right, o_left, o_across)

    w_stream.begin()
    wo_load.wait()
    at_end = (me == 0) | (me == n - 1)

    @pl.when(at_end)
    def _():
        o_stream.begin()

    tok_load.wait()

    row_step = 16

    def norm_rows(i, carry):
        rows = pl.ds(pl.multiple_of(i * row_step, row_step), row_step)
        sumsq = jnp.zeros((row_step, 1), F32)
        for c in range(2 * pieces):
            part = tok_ref[rows, c * span : (c + 1) * span].astype(F32)
            sumsq = sumsq + jnp.sum(part * part, axis=1, keepdims=True)
        scale = lax.rsqrt(sumsq / width + 1e-05)
        for c in range(2 * pieces):
            cols = slice(c * span, (c + 1) * span)
            part = tok_ref[rows, cols].astype(F32)
            normed[c, rows, :] = (part * scale * gain_ref[:, cols]).astype(BF16)
        return carry

    lax.fori_loop(0, tokens // row_step, norm_rows, 0)

    def contract(weights, acts):
        return lax.dot_general(weights, acts, (((1,), (1,)), ((), ())), preferred_element_type=F32)

    def qk_copy(o, source, other_f, token_block, f_from):
        return pltpu.make_async_remote_copy(
            src_ref=source,
            dst_ref=qk_all.at[token_block, f_from],
            send_sem=qk_ssem.at[o, other_f],
            recv_sem=qk_rsem.at[token_block, f_from],
            device_id={"seq": o, "fsdp": other_f},
            device_id_type=MESH,
        )

    def v_copy(o, token_block):
        return pltpu.make_async_remote_copy(
            src_ref=v_send.at[o],
            dst_ref=v_all.at[token_block],
            send_sem=v_ssem.at[o],
            recv_sem=v_rsem.at[token_block],
            device_id={"seq": o},
            device_id_type=MESH,
        )

    def project_own():
        acc = jnp.zeros((w_ref.shape[0], tokens), F32)
        for c in range(2 * pieces):
            acc = acc + contract(w_ref[:, c * span : (c + 1) * span], normed[c])
        qk_all[me, my_f] = acc[:qk_rows].astype(BF16)
        v_all[me] = acc[qk_rows:].astype(BF16)
        for df in range(1, nf):
            other = lax.rem(my_f + df, nf)
            qk_copy(me, qk_all.at[me, my_f], other, me, my_f).start()

    def project(o):
        def body(c, acc):
            return acc + contract(wbuf[o, c // pieces, c % pieces], normed[c])

        acc = lax.fori_loop(0, 2 * pieces, body, jnp.zeros((w_ref.shape[0], tokens), F32))
        qk_send[o] = acc[:qk_rows].astype(BF16)
        v_send[o] = acc[qk_rows:].astype(BF16)
        for df in range(nf):
            qk_copy(o, qk_send.at[o], lax.rem(my_f + df, nf), me, my_f).start()
        v_copy(o, me).start()

    def both(r, action):
        @pl.when(me >= r)
        def _():
            action(me - r)

        @pl.when(me + r < n)
        def _():
            action(me + r)

    def take(o):
        w_stream.arrive(o)
        project(o)

    project_own()
    for r in range(1, n):
        if r == n - 1:

            @pl.when(jnp.logical_not(at_end))
            def _():
                o_stream.begin()

        w_stream.relay(r, functools.partial(both, r - 1, take) if r > 1 else None)

    o_stream.relay(1, functools.partial(both, n - 1, take))

    def gather_heads():
        for d in range(1, n):
            t = lax.rem(me + d, n)
            v_copy(me, t).wait_recv()
            for df in range(nf):
                qk_copy(me, qk_all.at[t, df], 0, t, df).wait_recv()
        for df in range(1, nf):
            other = lax.rem(my_f + df, nf)
            qk_copy(me, qk_all.at[me, other], other, me, other).wait_recv()

        for t in range(n):
            parts = [qk_all[t, f].astype(F32) for f in range(nf)]
            q_full[t] = jnp.concatenate([p[:half_rows] for p in parts], 0).astype(BF16)
            k_full[t] = jnp.concatenate([p[half_rows:] for p in parts], 0).astype(BF16)

    channels = v_all.shape[1]
    key_pos = lax.broadcasted_iota(jnp.int32, (tokens, tokens), 0)
    query_pos = lax.broadcasted_iota(jnp.int32, (tokens, tokens), 1)

    def numerator(t):
        queries = q_full[t]

        def body(j, acc):
            scores = lax.dot_general(
                k_full[j], queries, (((0,), (0,)), ((), ())), preferred_element_type=F32
            )
            value = 1.0 + scores * 0.25 + scores * scores * 0.03125
            weight = jnp.where(key_pos + (j - t) * tokens <= query_pos, value, 0.0).astype(BF16)
            return acc + jnp.dot(v_all[j], weight, preferred_element_type=F32)

        acc = lax.fori_loop(0, t + 1, body, jnp.zeros((channels, tokens), F32))
        return acc.astype(BF16)

    def num_copy(t, head_block):
        return pltpu.make_async_remote_copy(
            src_ref=num_send.at[t],
            dst_ref=num_all.at[head_block, my_f, my_s],
            send_sem=num_ssem.at[t],
            recv_sem=num_rsem.at[head_block],
            device_id={"seq": t},
            device_id_type=MESH,
        )

    def sib_copy(o, to_f, to_s, from_f, from_s):
        slot = num_all.at[o, from_f, from_s]
        return pltpu.make_async_remote_copy(
            src_ref=slot,
            dst_ref=slot,
            send_sem=sib_ssem.at[o, to_f, to_s],
            recv_sem=sib_rsem.at[o, from_f, from_s],
            device_id={"fsdp": to_f, "sub": to_s},
            device_id_type=MESH,
        )

    def siblings():
        for df in range(nf):
            for ds in range(ns):
                if df or ds:
                    yield lax.rem(my_f + df, nf), lax.rem(my_s + ds, ns)

    def attend():
        gather_heads()
        for d in range(1, n):
            t = lax.rem(me + d, n)
            num_send[t] = numerator(t)
            num_copy(t, me).start()
        num_all[me, my_f, my_s] = numerator(me)
        for f, s in siblings():
            sib_copy(me, f, s, my_f, my_s).start()

    def spread():
        for d in range(1, n):
            o = lax.rem(me + d, n)
            num_copy(o, o).wait_recv()
            for f, s in siblings():
                sib_copy(o, f, s, my_f, my_s).start()

    for r in range(2, n):
        o_stream.relay(r, {2: attend, 3: spread}.get(r))

    for d in range(n):
        o = lax.rem(me + d, n)
        for f, s in siblings():
            sib_copy(o, f, s, f, s).wait_recv()

    head_width = nf * channels

    def attend_block(o, carry):
        for s in range(ns):
            whole = jnp.concatenate([num_all[o, f, s] for f in range(nf)], 0).astype(F32)
            meansq = jnp.sum(whole * whole, axis=0, keepdims=True) / head_width
            scaled = (whole * lax.rsqrt(meansq + 1e-06)).T * head_gain_ref[...]
            attended[o, :, s * head_width : (s + 1) * head_width] = scaled.astype(BF16)
        return carry

    lax.fori_loop(0, n, attend_block, 0)

    columns = out_ref.shape[1]
    depth = ns * head_width

    total[...] = jnp.dot(
        attended[me], wo_ref[...].reshape(depth, columns), preferred_element_type=F32
    )

    def multiply(o):
        o_stream.arrive(o)
        total[...] += jnp.dot(
            attended[o], wobuf[o].reshape(depth, columns), preferred_element_type=F32
        )

    for r in range(1, n):
        both(r, multiply)
    out_ref[...] = total[...].astype(BF16)

    w_stream.finish()
    o_stream.finish()
    for d in range(n):
        o = lax.rem(me + d, n)
        for df in range(nf):
            if d or df:
                other = lax.rem(my_f + df, nf)
                source = qk_send.at[o] if d else qk_all.at[me, my_f]
                qk_copy(o, source, other, me, my_f).wait_send()
        if d:
            v_copy(o, me).wait_send()
            num_copy(o, me).wait_send()
        for f, s in siblings():
            sib_copy(o, f, s, my_f, my_s).wait_send()


def per_device(sizes, tokens, norm_gain, w_query, w_key, w_value, head_gain, w_out):
    n, nf, ns = sizes
    shards = [w_query[0], w_key[0], w_value[0]]
    if any(shard.shape[0] % 8 for shard in shards):
        shards = [jnp.concatenate(shards, 0)]
    rows, width = sum(shard.shape[0] for shard in shards), tokens.shape[1]
    count = tokens.shape[0]
    qk_rows = w_query.shape[1] + w_key.shape[1]
    channels = w_value.shape[1]
    head_width, columns = w_out.shape[1], w_out.shape[2]
    pieces = max(1, 16 // n)
    out_pieces = max(1, 16 // n)
    wo = w_out.reshape(ns, out_pieces, head_width // out_pieces, columns)
    hbm = pl.BlockSpec(memory_space=pl.ANY)
    vmem = pl.BlockSpec(memory_space=pltpu.VMEM)
    dma = pltpu.SemaphoreType.DMA
    return pl.pallas_call(
        functools.partial(kernel, n, nf, ns, pieces, out_pieces, len(shards)),
        out_shape=jax.ShapeDtypeStruct((count, columns), BF16),
        in_specs=[hbm, vmem, vmem, hbm] + [hbm] * len(shards),
        out_specs=vmem,
        scratch_shapes=[
            pltpu.VMEM(tokens.shape, BF16),
            pltpu.VMEM((rows, width), BF16),
            pltpu.VMEM(wo.shape, BF16),
            dma((len(shards) + 2,)),
            pltpu.VMEM((2 * pieces, count, width // (2 * pieces)), BF16),
            pltpu.VMEM((n, 2, pieces, rows, width // (2 * pieces)), BF16),
            pltpu.VMEM((n,) + wo.shape, BF16),
            pltpu.VMEM((n, qk_rows, count), BF16),
            pltpu.VMEM((n, channels, count), BF16),
            pltpu.VMEM((n, nf, qk_rows, count), BF16),
            pltpu.VMEM((n, channels, count), BF16),
            pltpu.VMEM((n, nf * qk_rows // 2, count), BF16),
            pltpu.VMEM((n, nf * qk_rows // 2, count), BF16),
            pltpu.VMEM((n, channels, count), BF16),
            pltpu.VMEM((n, nf, ns, channels, count), BF16),
            pltpu.VMEM((n, count, ns * head_width), BF16),
            pltpu.VMEM((count, columns), F32),
        ]
        + [dma((n, pieces))] * 5
        + [dma((n, out_pieces))] * 5
        + [
            dma((n, nf)),
            dma((n, nf)),
            dma((n,)),
            dma((n,)),
            dma((n,)),
            dma((n,)),
            dma((n, nf, ns)),
            dma((n, nf, ns)),
        ],
        compiler_params=pltpu.CompilerParams(
            collective_id=0, has_side_effects=True, vmem_limit_bytes=60 * 1024 * 1024
        ),
    )(tokens, norm_gain.reshape(1, -1), head_gain.reshape(1, -1), wo, *shards)


def solution(mesh):
    in_specs = (
        P(("groups", "seq"), None),
        P(),
        P(("seq", "sub"), "fsdp", None),
        P(("seq", "sub"), "fsdp", None),
        P(("seq", "sub"), "fsdp", None),
        P(),
        P("seq", None, ("fsdp", "sub")),
    )
    out_specs = P(("groups", "seq"), ("fsdp", "sub"))
    sizes = (mesh.shape["seq"], mesh.shape["fsdp"], mesh.shape["sub"])
    return jax.shard_map(
        functools.partial(per_device, sizes),
        mesh=mesh,
        in_specs=in_specs,
        out_specs=out_specs,
        check_vma=False,
    )
```
